128 devices in a mesh: dp: 128 (over x, z, y, core).
Axes of the slice: x: 4, y: 4, z: 4, core: 2. Of those that a mesh axis runs over, the one named last changes fastest.
Arguments:
- grads: float32 [128, 8192, 128], P('dp'), may hold values from -6 to 6
- error: float32 [128, 8192, 128], P('dp'), may hold values from -4 to 4
- picks: int32 [128, 32], P('dp'), may hold values from 0 to 8191, as said below
- owned_ids: int32 [8192], P('dp'), may hold values from 0 to 8191, as said below
- params: float32 [8192, 128], P('dp'), may hold values from -6 to 6
- momentum: float32 [8192, 128], P('dp'), may hold values from -6 to 6
Outputs:
- new_error: float32 [128, 8192, 128], P('dp')
- new_params: float32 [8192, 128], P('dp')
- new_momentum: float32 [8192, 128], P('dp')
The draws below stay inside these ranges and needn't reach their ends.
Inputs may be any that keep to these rules, and one draw needn't show every extreme that they name: `picks`: each row holds 32 different block numbers; at most 4 of a row's blocks lie in the slots of one device, and one device's slots hold exactly 4 blocks of every row. `owned_ids`: every block number appears once.
All inputs are finite; a program needn't handle non-finite values.
Results may differ from the reference program's by a relative error of at most 0.000064.
Values sent between devices are 32-bit elements; how exact they have to be, the bound alone decides.
No kernel may reach another device: no remote copies, remote signals or barrier semaphores. Data moves between devices by JAX's collectives and lax.ppermute only.
A program may use at most 64 MiB of HBM per device.

```python
import jax
import jax.numpy as jnp
from jax import lax

BLOCK = 128
BLK_OWN = 64
PARAMETER_BLOCKS = 8192
K = 32
CAP = 4
N_DP = 128


def shared_draw(key):
    base = jax.random.fold_in(key, 11)
    perm_key, hot_key, owner_key, row_key = jax.random.split(base, 4)
    owned = jax.random.permutation(perm_key, PARAMETER_BLOCKS).astype(jnp.int32)
    slot_holder_index = jnp.arange(PARAMETER_BLOCKS, dtype=jnp.int32) // BLK_OWN
    order = jax.random.permutation(hot_key, PARAMETER_BLOCKS)
    block_heat = (order < PARAMETER_BLOCKS // 8).astype(jnp.int32)
    preferred_blocks = jax.random.randint(owner_key, (), 0, N_DP)
    extra_credit = 100 * (slot_holder_index == preferred_blocks).astype(jnp.int32)
    row_keys = jax.random.split(row_key, N_DP)

    def one_row(single):
        leading_entry, second, third = jax.random.split(single, 3)
        unscaled_gradient = jax.random.randint(leading_entry, (PARAMETER_BLOCKS,), 0, 6) + 3 * block_heat + extra_credit
        tiebreak = jax.random.permutation(second, PARAMETER_BLOCKS).astype(jnp.int32)
        priority = jax.random.permutation(third, PARAMETER_BLOCKS).astype(jnp.int32).reshape(N_DP, BLK_OWN)
        ranks = jnp.argsort(jnp.argsort(priority, axis=1, stable=True), axis=1, stable=True).reshape(PARAMETER_BLOCKS)
        scores = jnp.where(ranks < CAP, unscaled_gradient * PARAMETER_BLOCKS + tiebreak, -1)
        unused, slots = lax.top_k(scores, K)
        return jnp.take(owned, slots.astype(jnp.int32), axis=0).astype(jnp.int32)
    return (owned, jax.vmap(one_row)(row_keys))


def draw_picks(key, part):
    return shared_draw(key)[1]


def draw_owned_ids(key, part):
    return shared_draw(key)[0]


def block_levels(key, extent, cuts, smallest, largest):
    factor_of = 1.0
    for axis_at, parts in cuts:
        draws = jax.random.uniform(jax.random.fold_in(jax.random.fold_in(key, 6), axis_at), (parts,), jnp.float32, smallest / len(cuts), largest / len(cuts))
        factor_of = factor_of * jnp.repeat(jnp.exp(draws), extent[axis_at] // parts).reshape((-1,) + (1,) * (len(extent) - 1 - axis_at))
    return factor_of


def normal_values(stream_key, dims, deviation, most, cuts=(), kind=jnp.bfloat16):
    array = jax.random.normal(stream_key, dims, jnp.float32) * deviation
    if len(cuts) > 0:
        array = block_levels(stream_key, dims, cuts, -0.22, 0.18) * array
    return jnp.clip(array, min=-most, max=most).astype(kind)


def setup_inputs(seed: int = 0) -> dict:
    key_of = jax.random.split(jax.random.key(seed), 7)
    return {
        "grads": normal_values(key_of[0], (N_DP, PARAMETER_BLOCKS, BLOCK), 1.0, 6.0, ((0, 128),), jnp.float32),
        "error": normal_values(key_of[1], (N_DP, PARAMETER_BLOCKS, BLOCK), 0.5, 4.0, ((0, 128),), jnp.float32),
        "picks": draw_picks(jax.random.fold_in(key_of[6], 71), 0),
        "owned_ids": draw_owned_ids(jax.random.fold_in(key_of[6], 71), 0),
        "params": normal_values(key_of[4], (PARAMETER_BLOCKS, BLOCK), 1.0, 6.0, ((0, 128),), jnp.float32),
        "momentum": normal_values(key_of[5], (PARAMETER_BLOCKS, BLOCK), 1.0, 6.0, ((0, 128),), jnp.float32),
    }


def reference(grads, error, picks, owned_ids, params, momentum):
    acc = grads + error
    rows = jnp.arange(picks.shape[0], dtype=jnp.int32)[:, None]
    keep = jnp.zeros((picks.shape[0], acc.shape[1]), jnp.float32).at[rows, picks].set(1.0)
    new_error = acc * (1.0 - keep)[:, :, None]
    total = jnp.sum(acc * keep[:, :, None], axis=0)
    owned_total = jnp.take(total, owned_ids, axis=0)
    new_momentum = 0.9 * momentum + owned_total
    new_params = params - 0.5 * new_momentum
    return new_error, new_params, new_momentum
```

```python
import jax
import jax.numpy as jnp
from jax import lax
from jax.experimental import pallas as pl
from jax.experimental.pallas import tpu as pltpu
from jax.sharding import Mesh
from jax.sharding import PartitionSpec as P

DP = ("x", "z", "yh", "yl", "c")
GATHER = ("x", "z", "yh")
SERVE = ("yl", "c")
PEERS = 32
LANES = 128
STEP = 1024


def xor_pairs(bits):
    return [(i, i ^ bits) for i in range(4)]


def rows_kernel(picks_hbm, grads, error, out, picks, gbuf, ebuf, psem, gsem, esem):
    fetch = pltpu.make_async_copy(picks_hbm, picks, psem)
    fetch.start()
    fetch.wait()
    count = picks.shape[0]
    for k in range(count):
        row = picks[k]
        pltpu.make_async_copy(grads.at[pl.ds(row, 1)], gbuf.at[pl.ds(k, 1)], gsem).start()
        pltpu.make_async_copy(error.at[pl.ds(row, 1)], ebuf.at[pl.ds(k, 1)], esem).start()
    lane = lax.broadcasted_iota(jnp.int32, (1, LANES), 1) % count
    ids = jnp.zeros((1, LANES), jnp.int32)
    for k in range(count):
        ids = jnp.where(lane == k, picks[k], ids)
    pltpu.make_async_copy(grads.at[pl.ds(0, count)], gbuf, gsem).wait()
    pltpu.make_async_copy(error.at[pl.ds(0, count)], ebuf, esem).wait()
    acc = gbuf[:, 0, :] + ebuf[:, 0, :]
    ids = ids.astype(jnp.float32)
    for p in range(PEERS):
        base = p * (count + 1)
        out[base : base + count, :] = acc
        out[base + count : base + count + 1, :] = ids


def chosen_rows(picks, grads, error):
    count = picks.shape[0]
    return pl.pallas_call(
        rows_kernel,
        in_specs=[pl.BlockSpec(memory_space=pltpu.HBM)] * 3,
        scratch_shapes=[
            pltpu.SMEM((count,), jnp.int32),
            pltpu.VMEM((count, 1, LANES), jnp.float32),
            pltpu.VMEM((count, 1, LANES), jnp.float32),
            pltpu.SemaphoreType.DMA,
            pltpu.SemaphoreType.DMA,
            pltpu.SemaphoreType.DMA,
        ],
        out_shape=jax.ShapeDtypeStruct((PEERS * (count + 1), LANES), jnp.float32),
        name="chosen_rows",
    )(picks, grads.reshape(-1, 1, LANES), error.reshape(-1, 1, LANES))


def dense_kernel(picks, grads, error, out):
    out[...] = grads[...] + error[...]
    start = pl.program_id(0) * STEP
    for k in range(picks.shape[0]):
        row = picks[k] - start

        @pl.when((row >= 0) & (row < STEP))
        def _():
            out[pl.ds(row, 1), :] = jnp.zeros((1, LANES), jnp.float32)


def remainder(picks, grads, error):
    blocks = grads.shape[0]
    spec = pl.BlockSpec((STEP, LANES), lambda i, p: (i, 0))
    return pl.pallas_call(
        dense_kernel,
        grid_spec=pltpu.PrefetchScalarGridSpec(
            num_scalar_prefetch=1,
            grid=(blocks // STEP,),
            in_specs=[spec, spec],
            out_specs=spec,
        ),
        out_shape=jax.ShapeDtypeStruct(grads.shape, jnp.float32),
        cost_estimate=pl.CostEstimate(
            flops=40_000_000, bytes_accessed=12 << 20, transcendentals=0
        ),
        name="remainder",
    )(picks, grads, error)


def totals_kernel(got, id0, id1, id2, id3, out0, out1, out2, out3):
    count = got.shape[0] // PEERS - 1
    per = LANES // count
    lane = lax.broadcasted_iota(jnp.int32, (1, LANES), 1)
    slots = id0.shape[1]
    columns = []
    for ids in (id0, id1, id2, id3):
        wide = jnp.broadcast_to(ids[...].astype(jnp.float32), (LANES, slots))
        columns.append(wide.T)
    owned = jnp.concatenate(columns, axis=0)
    marks, values = [], []
    for g in range(PEERS // per):
        ids = None
        for q in range(per):
            base = (g * per + q) * (count + 1)
            row = got[base + count : base + count + 1, :]
            ids = row if ids is None else jnp.where(lane < q * count, ids, row)
            values.append(got[base : base + count, :])
        marks.append(jnp.where(owned == ids, 1.0, 0.0).astype(jnp.bfloat16))
    marks = jnp.concatenate(marks, axis=1)
    values = jnp.concatenate(values, axis=0)
    total = None
    for _ in range(3):
        part = values.astype(jnp.bfloat16)
        values = values - part.astype(jnp.float32)
        term = jnp.dot(marks, part, preferred_element_type=jnp.float32)
        total = term if total is None else total + term
    for j, out in enumerate((out0, out1, out2, out3)):
        out[...] = total[j * slots : (j + 1) * slots, :]


def totals(got, ids):
    slots = ids[0].shape[1]
    return pl.pallas_call(
        totals_kernel,
        out_shape=[jax.ShapeDtypeStruct((slots, LANES), jnp.float32)] * 4,
        compiler_params=pltpu.CompilerParams(vmem_limit_bytes=8 << 20),
        name="totals",
    )(got, *ids)


def update_kernel(momentum, params, a, b, c, d, new_params, new_momentum):
    fresh = 0.9 * momentum[...] + ((a[...] + b[...]) + (c[...] + d[...]))
    new_momentum[...] = fresh
    new_params[...] = params[...] - 0.5 * fresh


def update(momentum, params, parts):
    shape = jax.ShapeDtypeStruct(params.shape, jnp.float32)
    return pl.pallas_call(
        update_kernel,
        out_shape=[shape, shape],
        compiler_params=pltpu.CompilerParams(vmem_limit_bytes=2 << 20),
        name="update",
    )(momentum, params, *parts)


def on_device(grads, error, picks, owned_ids, params, momentum):
    grads, error, picks = grads[0], error[0], picks[0]
    count = picks.shape[0]
    send = chosen_rows(picks, grads, error)
    send = send.reshape(PEERS, count + 1, 1, LANES)
    got = lax.all_to_all(send, GATHER, 0, 0, tiled=True)
    mine = owned_ids.reshape(1, -1)
    ids = [mine] + [lax.ppermute(mine, SERVE, xor_pairs(b)) for b in (1, 2, 3)]
    new_error = remainder(picks, grads, error)
    got, new_error = lax.optimization_barrier((got, new_error))
    parts = totals(got.reshape(-1, LANES), ids)
    parts = [parts[0]] + [lax.ppermute(parts[b], SERVE, xor_pairs(b)) for b in (1, 2, 3)]
    new_params, new_momentum = update(momentum, params, parts)
    return new_error[None], new_params, new_momentum


def solution(mesh):
    split = Mesh(mesh.devices.reshape(4, 4, 2, 2, 2), DP)
    return jax.shard_map(
        on_device,
        mesh=split,
        in_specs=(
            P(DP, None, None),
            P(DP, None, None),
            P(DP, None),
            P(DP),
            P(DP, None),
            P(DP, None),
        ),
        out_specs=(P(DP, None, None), P(DP, None), P(DP, None)),
        check_vma=False,
    )
```

```python
import jax
import jax.numpy as jnp
from jax import lax
from jax.experimental import pallas as pl
from jax.experimental.pallas import tpu as pltpu
from jax.sharding import Mesh
from jax.sharding import PartitionSpec as P

DP = ("x", "z", "y", "c")
GATHER = ("x", "z")
SERVE = "y"
PEERS = 16
LANES = 128
STEP = 1024
CHUNKS = 8
EARLY = 5


def xor_pairs(bits):
    return [(i, i ^ bits) for i in range(4)]


def early_chunks():
    far = lax.axis_index("x") + lax.axis_index("z") + lax.axis_index("y")
    return jnp.clip(EARLY - far, 0, CHUNKS)


def chunk_loads(i, grads, error, gbuf, ebuf, gsem, esem):
    rows = pl.ds(i * STEP, STEP)
    return (
        pltpu.make_async_copy(grads.at[rows], gbuf.at[rows], gsem.at[i]),
        pltpu.make_async_copy(error.at[rows], ebuf.at[rows], esem.at[i]),
    )


def chunk_store(i, obuf, out, osem):
    rows = pl.ds(i * STEP, STEP)
    return pltpu.make_async_copy(obuf.at[i, pl.ds(0, STEP)], out.at[rows], osem.at[i])


def chunk_work(i, picks, gbuf, ebuf, obuf):
    rows = pl.ds(i * STEP, STEP)
    obuf[i, pl.ds(0, STEP), :] = gbuf[rows, :] + ebuf[rows, :]
    for k in range(picks.shape[0]):
        row = picks[k] - i * STEP
        row = jnp.where((row >= 0) & (row < STEP), row, STEP)
        obuf[i, pl.ds(row, 1), :] = jnp.zeros((1, LANES), jnp.float32)


def dense_chunks(wanted, picks, grads, error, out, gbuf, ebuf, obuf, gsem, esem, osem, first):
    for i in range(CHUNKS):

        @pl.when(wanted(i))
        def _():
            for copy in chunk_loads(i, grads, error, gbuf, ebuf, gsem, esem):
                copy.start()

    first()
    for i in range(CHUNKS):

        @pl.when(wanted(i))
        def _():
            for copy in chunk_loads(i, grads, error, gbuf, ebuf, gsem, esem):
                copy.wait()
            chunk_work(i, picks, gbuf, ebuf, obuf)
            chunk_store(i, obuf, out, osem).start()

    for i in range(CHUNKS):

        @pl.when(wanted(i))
        def _():
            chunk_store(i, obuf, out, osem).wait()


def dense_scratch(blocks):
    return [
        pltpu.VMEM((blocks, LANES), jnp.float32),
        pltpu.VMEM((blocks, LANES), jnp.float32),
        pltpu.VMEM((CHUNKS, STEP + 8, LANES), jnp.float32),
        pltpu.SemaphoreType.DMA((CHUNKS,)),
        pltpu.SemaphoreType.DMA((CHUNKS,)),
        pltpu.SemaphoreType.DMA((CHUNKS,)),
    ]


def rows_kernel(
    picks_hbm, grads, error, grads_rows, error_rows, send, out,
    picks, grow, erow, psem, rsem, ssem, gbuf, ebuf, obuf, gsem, esem, osem,
):
    fetch = pltpu.make_async_copy(picks_hbm, picks, psem)
    fetch.start()
    fetch.wait()
    count = picks.shape[0]
    for k in range(count):
        row = picks[k]
        pltpu.make_async_copy(grads_rows.at[pl.ds(row, 1)], grow.at[pl.ds(k, 1)], rsem).start()
        pltpu.make_async_copy(error_rows.at[pl.ds(row, 1)], erow.at[pl.ds(k, 1)], ssem).start()
    limit = early_chunks()

    def build():
        lane = lax.broadcasted_iota(jnp.int32, (1, LANES), 1) % count
        ids = jnp.zeros((1, LANES), jnp.int32)
        for k in range(count):
            ids = jnp.where(lane == k, picks[k], ids)
        pltpu.make_async_copy(grads_rows.at[pl.ds(0, count)], grow, rsem).wait()
        pltpu.make_async_copy(error_rows.at[pl.ds(0, count)], erow, ssem).wait()
        acc = grow[:, 0, :] + erow[:, 0, :]
        ids = ids.astype(jnp.float32)
        for p in range(PEERS):
            base = p * (count + 1)
            send[base : base + count, :] = acc
            send[base + count : base + count + 1, :] = ids

    dense_chunks(
        lambda i: i < limit, picks, grads, error, out, gbuf, ebuf, obuf, gsem, esem, osem, build
    )


def chosen_rows(picks, grads, error):
    count = picks.shape[0]
    return pl.pallas_call(
        rows_kernel,
        in_specs=[pl.BlockSpec(memory_space=pltpu.HBM)] * 5,
        out_specs=[pl.BlockSpec(memory_space=pltpu.VMEM), pl.BlockSpec(memory_space=pltpu.HBM)],
        scratch_shapes=[
            pltpu.SMEM((count,), jnp.int32),
            pltpu.VMEM((count, 1, LANES), jnp.float32),
            pltpu.VMEM((count, 1, LANES), jnp.float32),
            pltpu.SemaphoreType.DMA,
            pltpu.SemaphoreType.DMA,
            pltpu.SemaphoreType.DMA,
        ]
        + dense_scratch(grads.shape[0]),
        out_shape=[
            jax.ShapeDtypeStruct((PEERS * (count + 1), LANES), jnp.float32),
            jax.ShapeDtypeStruct(grads.shape, jnp.float32),
        ],
        name="chosen_rows",
    )(picks, grads, error, grads.reshape(-1, 1, LANES), error.reshape(-1, 1, LANES))


def late_kernel(
    picks_hbm, grads, error, begun, out,
    picks, psem, gbuf, ebuf, obuf, gsem, esem, osem,
):
    limit = early_chunks()

    @pl.when(limit < CHUNKS)
    def _():
        fetch = pltpu.make_async_copy(picks_hbm, picks, psem)
        fetch.start()
        dense_chunks(
            lambda i: i >= limit,
            picks, grads, error, out, gbuf, ebuf, obuf, gsem, esem, osem, fetch.wait,
        )


def remainder(picks, grads, error, begun):
    return pl.pallas_call(
        late_kernel,
        in_specs=[pl.BlockSpec(memory_space=pltpu.HBM)] * 4,
        out_specs=pl.BlockSpec(memory_space=pltpu.HBM),
        out_shape=jax.ShapeDtypeStruct(grads.shape, jnp.float32),
        input_output_aliases={3: 0},
        scratch_shapes=[pltpu.SMEM(picks.shape, jnp.int32), pltpu.SemaphoreType.DMA]
        + dense_scratch(grads.shape[0]),
        cost_estimate=pl.CostEstimate(
            flops=40_000_000, bytes_accessed=12 << 20, transcendentals=0
        ),
        name="remainder",
    )(picks, grads, error, begun)


def totals_kernel(mine, other, id0, id1, id2, id3, out0, out1, out2, out3):
    count = mine.shape[0] // PEERS - 1
    per = LANES // count
    lane = lax.broadcasted_iota(jnp.int32, (1, LANES), 1)
    slots = id0.shape[1]
    columns = []
    for ids in (id0, id1, id2, id3):
        wide = jnp.broadcast_to(ids[...].astype(jnp.float32), (LANES, slots))
        columns.append(wide.T)
    owned = jnp.concatenate(columns, axis=0)
    marks, values = [], []
    for g in range(2 * PEERS // per):
        ids = None
        got = mine if g < PEERS // per else other
        for q in range(per):
            base = (g * per + q) % PEERS * (count + 1)
            row = got[base + count : base + count + 1, :]
            ids = row if ids is None else jnp.where(lane < q * count, ids, row)
            values.append(got[base : base + count, :])
        marks.append(jnp.where(owned == ids, 1.0, 0.0).astype(jnp.bfloat16))
    marks = jnp.concatenate(marks, axis=1)
    values = jnp.concatenate(values, axis=0)
    total = None
    for _ in range(3):
        part = values.astype(jnp.bfloat16)
        values = values - part.astype(jnp.float32)
        term = jnp.dot(marks, part, preferred_element_type=jnp.float32)
        total = term if total is None else total + term
    for j, out in enumerate((out0, out1, out2, out3)):
        out[...] = total[j * slots : (j + 1) * slots, :]


def totals(mine, other, ids):
    slots = ids[0].shape[1]
    return pl.pallas_call(
        totals_kernel,
        out_shape=[jax.ShapeDtypeStruct((slots, LANES), jnp.float32)] * 4,
        compiler_params=pltpu.CompilerParams(vmem_limit_bytes=8 << 20),
        name="totals",
    )(mine, other, *ids)


def update_kernel(momentum, params, a, b, c, d, new_params, new_momentum):
    fresh = 0.9 * momentum[...] + ((a[...] + b[...]) + (c[...] + d[...]))
    new_momentum[...] = fresh
    new_params[...] = params[...] - 0.5 * fresh


def update(momentum, params, parts):
    shape = jax.ShapeDtypeStruct(params.shape, jnp.float32)
    return pl.pallas_call(
        update_kernel,
        out_shape=[shape, shape],
        compiler_params=pltpu.CompilerParams(vmem_limit_bytes=2 << 20),
        name="update",
    )(momentum, params, *parts)


def swapped(x, bits):
    return lax.ppermute(x, SERVE, xor_pairs(bits))


def on_device(grads, error, picks, owned_ids, params, momentum):
    return step(grads[0], error[0], picks[0], owned_ids, params, momentum)


def step(grads, error, picks, owned_ids, params, momentum):
    count = picks.shape[0]
    send, begun = chosen_rows(picks, grads, error)
    send = send.reshape(PEERS, count + 1, 1, LANES)
    got = lax.all_to_all(send, GATHER, 0, 0, tiled=True)
    mine = owned_ids.reshape(1, -1)
    ids = [mine] + [swapped(mine, b) for b in (1, 2, 3)]
    got = got.reshape(-1, LANES)
    other = lax.ppermute(got, "c", [(0, 1), (1, 0)])
    parts = totals(got, other, ids)
    new_error = remainder(picks, grads, error, begun)
    parts = [parts[0]] + [swapped(parts[b], b) for b in (1, 2, 3)]
    new_params, new_momentum = update(momentum, params, parts)
    return new_error[None], new_params, new_momentum


def solution(mesh):
    split = Mesh(mesh.devices.reshape(4, 4, 4, 2), DP)
    return jax.shard_map(
        on_device,
        mesh=split,
        in_specs=(
            P(DP, None, None),
            P(DP, None, None),
            P(DP, None),
            P(DP),
            P(DP, None),
            P(DP, None),
        ),
        out_specs=(P(DP, None, None), P(DP, None), P(DP, None)),
        check_vma=False,
    )
```

```python
import jax
import jax.numpy as jnp
from jax import lax
from jax.experimental import pallas as pl
from jax.experimental.pallas import tpu as pltpu
from jax.sharding import PartitionSpec as P

DP = "dp"
PEERS = 16
LANES = 128
STEP = 1024
CHUNKS = 8
EARLY = 5


def rank(x, z, y, c):
    return ((x * 4 + z) * 4 + y) * 2 + c


def partners(zbits, cbits):
    ranks = range(128)
    return [(i, i ^ (zbits * 8) ^ cbits) for i in ranks]


def planes():
    order = [(x, y) for x in range(4) for y in range(4)]
    order = sorted(order, key=lambda p: (p != (2, 2), -p[0], -p[1]))
    return [[rank(x, z, y, c) for x, y in order] for z in range(4) for c in range(2)]


def early_chunks():
    here = lax.axis_index(DP)
    far = here // 32 + here // 8 % 4 + here // 2 % 4
    return jnp.clip(EARLY - far, 0, CHUNKS)


def chunk_loads(i, grads, error, gbuf, ebuf, gsem, esem):
    rows = pl.ds(i * STEP, STEP)
    return (
        pltpu.make_async_copy(grads.at[rows], gbuf.at[rows], gsem.at[i]),
        pltpu.make_async_copy(error.at[rows], ebuf.at[rows], esem.at[i]),
    )


def chunk_store(i, obuf, out, osem):
    rows = pl.ds(i * STEP, STEP)
    return pltpu.make_async_copy(obuf.at[i, pl.ds(0, STEP)], out.at[rows], osem.at[i])


def chunk_work(i, picks, gbuf, ebuf, obuf):
    rows = pl.ds(i * STEP, STEP)
    obuf[i, pl.ds(0, STEP), :] = gbuf[rows, :] + ebuf[rows, :]
    for k in range(picks.shape[0]):
        row = picks[k] - i * STEP
        row = jnp.where((row >= 0) & (row < STEP), row, STEP)
        obuf[i, pl.ds(row, 1), :] = jnp.zeros((1, LANES), jnp.float32)


def dense_chunks(wanted, picks, grads, error, out, gbuf, ebuf, obuf, gsem, esem, osem, first):
    for i in range(CHUNKS):

        @pl.when(wanted(i))
        def _():
            for copy in chunk_loads(i, grads, error, gbuf, ebuf, gsem, esem):
                copy.start()

    first()
    for i in range(CHUNKS):

        @pl.when(wanted(i))
        def _():
            for copy in chunk_loads(i, grads, error, gbuf, ebuf, gsem, esem):
                copy.wait()
            chunk_work(i, picks, gbuf, ebuf, obuf)
            chunk_store(i, obuf, out, osem).start()

    for i in range(CHUNKS):

        @pl.when(wanted(i))
        def _():
            chunk_store(i, obuf, out, osem).wait()


def dense_scratch(blocks):
    return [
        pltpu.VMEM((blocks, LANES), jnp.float32),
        pltpu.VMEM((blocks, LANES), jnp.float32),
        pltpu.VMEM((CHUNKS, STEP + 8, LANES), jnp.float32),
        pltpu.SemaphoreType.DMA((CHUNKS,)),
        pltpu.SemaphoreType.DMA((CHUNKS,)),
        pltpu.SemaphoreType.DMA((CHUNKS,)),
    ]


def rows_kernel(
    picks_hbm, grads, error, grads_rows, error_rows, send, out,
    picks, grow, erow, psem, rsem, ssem, gbuf, ebuf, obuf, gsem, esem, osem,
):
    fetch = pltpu.make_async_copy(picks_hbm, picks, psem)
    fetch.start()
    fetch.wait()
    count = picks.shape[0]
    for k in range(count):
        row = picks[k]
        pltpu.make_async_copy(grads_rows.at[pl.ds(row, 1)], grow.at[pl.ds(k, 1)], rsem).start()
        pltpu.make_async_copy(error_rows.at[pl.ds(row, 1)], erow.at[pl.ds(k, 1)], ssem).start()
    limit = early_chunks()

    def build():
        lane = lax.broadcasted_iota(jnp.int32, (1, LANES), 1) % count
        ids = jnp.zeros((1, LANES), jnp.int32)
        for k in range(count):
            ids = jnp.where(lane == k, picks[k], ids)
        pltpu.make_async_copy(grads_rows.at[pl.ds(0, count)], grow, rsem).wait()
        pltpu.make_async_copy(error_rows.at[pl.ds(0, count)], erow, ssem).wait()
        acc = grow[:, 0, :] + erow[:, 0, :]
        ids = ids.astype(jnp.float32)
        for p in range(PEERS):
            base = p * (count + 1)
            send[base : base + count, :] = acc
            send[base + count : base + count + 1, :] = ids

    dense_chunks(
        lambda i: i < limit, picks, grads, error, out, gbuf, ebuf, obuf, gsem, esem, osem, build
    )


def chosen_rows(picks, grads, error):
    count = picks.shape[0]
    return pl.pallas_call(
        rows_kernel,
        in_specs=[pl.BlockSpec(memory_space=pltpu.HBM)] * 5,
        out_specs=[pl.BlockSpec(memory_space=pltpu.VMEM), pl.BlockSpec(memory_space=pltpu.HBM)],
        scratch_shapes=[
            pltpu.SMEM((count,), jnp.int32),
            pltpu.VMEM((count, 1, LANES), jnp.float32),
            pltpu.VMEM((count, 1, LANES), jnp.float32),
            pltpu.SemaphoreType.DMA,
            pltpu.SemaphoreType.DMA,
            pltpu.SemaphoreType.DMA,
        ]
        + dense_scratch(grads.shape[0]),
        out_shape=[
            jax.ShapeDtypeStruct((PEERS * (count + 1), LANES), jnp.float32),
            jax.ShapeDtypeStruct(grads.shape, jnp.float32),
        ],
        name="chosen_rows",
    )(picks, grads, error, grads.reshape(-1, 1, LANES), error.reshape(-1, 1, LANES))


def late_kernel(
    picks_hbm, grads, error, begun, out,
    picks, psem, gbuf, ebuf, obuf, gsem, esem, osem,
):
    limit = early_chunks()

    @pl.when(limit < CHUNKS)
    def _():
        fetch = pltpu.make_async_copy(picks_hbm, picks, psem)
        fetch.start()
        dense_chunks(
            lambda i: i >= limit,
            picks, grads, error, out, gbuf, ebuf, obuf, gsem, esem, osem, fetch.wait,
        )


def remainder(picks, grads, error, begun):
    return pl.pallas_call(
        late_kernel,
        in_specs=[pl.BlockSpec(memory_space=pltpu.HBM)] * 4,
        out_specs=pl.BlockSpec(memory_space=pltpu.HBM),
        out_shape=jax.ShapeDtypeStruct(grads.shape, jnp.float32),
        input_output_aliases={3: 0},
        scratch_shapes=[pltpu.SMEM(picks.shape, jnp.int32), pltpu.SemaphoreType.DMA]
        + dense_scratch(grads.shape[0]),
        cost_estimate=pl.CostEstimate(
            flops=40_000_000, bytes_accessed=12 << 20, transcendentals=0
        ),
        name="remainder",
    )(picks, grads, error, begun)


def totals_kernel(mine, other, id0, id1, id2, id3, out0, out1, out2, out3):
    count = mine.shape[0] // PEERS - 1
    per = LANES // count
    lane = lax.broadcasted_iota(jnp.int32, (1, LANES), 1)
    slots = id0.shape[1]
    columns = []
    for ids in (id0, id1, id2, id3):
        wide = jnp.broadcast_to(ids[...].astype(jnp.float32), (LANES, slots))
        columns.append(wide.T)
    owned = jnp.concatenate(columns, axis=0)
    marks, values = [], []
    for g in range(2 * PEERS // per):
        ids = None
        got = mine if g < PEERS // per else other
        for q in range(per):
            base = (g * per + q) % PEERS * (count + 1)
            row = got[base + count : base + count + 1, :]
            ids = row if ids is None else jnp.where(lane < q * count, ids, row)
            values.append(got[base : base + count, :])
        marks.append(jnp.where(owned == ids, 1.0, 0.0).astype(jnp.bfloat16))
    marks = jnp.concatenate(marks, axis=1)
    values = jnp.concatenate(values, axis=0)
    total = None
    for _ in range(3):
        part = values.astype(jnp.bfloat16)
        values = values - part.astype(jnp.float32)
        term = jnp.dot(marks, part, preferred_element_type=jnp.float32)
        total = term if total is None else total + term
    for j, out in enumerate((out0, out1, out2, out3)):
        out[...] = total[j * slots : (j + 1) * slots, :]


def totals(mine, other, ids):
    slots = ids[0].shape[1]
    return pl.pallas_call(
        totals_kernel,
        out_shape=[jax.ShapeDtypeStruct((slots, LANES), jnp.float32)] * 4,
        compiler_params=pltpu.CompilerParams(vmem_limit_bytes=8 << 20),
        name="totals",
    )(mine, other, *ids)


def update_kernel(momentum, params, a, b, c, d, new_params, new_momentum):
    fresh = 0.9 * momentum[...] + ((a[...] + b[...]) + (c[...] + d[...]))
    new_momentum[...] = fresh
    new_params[...] = params[...] - 0.5 * fresh


def update(momentum, params, parts):
    shape = jax.ShapeDtypeStruct(params.shape, jnp.float32)
    return pl.pallas_call(
        update_kernel,
        out_shape=[shape, shape],
        compiler_params=pltpu.CompilerParams(vmem_limit_bytes=2 << 20),
        name="update",
    )(momentum, params, *parts)


def swapped(x, bits):
    return lax.ppermute(x, DP, partners(bits, 0))


def on_device(grads, error, picks, owned_ids, params, momentum):
    return step(grads[0], error[0], picks[0], owned_ids, params, momentum)


def step(grads, error, picks, owned_ids, params, momentum):
    count = picks.shape[0]
    send, begun = chosen_rows(picks, grads, error)
    send = send.reshape(PEERS, count + 1, 1, LANES)
    got = lax.all_to_all(send, DP, 0, 0, tiled=True, axis_index_groups=planes())
    mine = owned_ids.reshape(1, -1)
    ids = [mine] + [swapped(mine, b) for b in (1, 2, 3)]
    got = got.reshape(-1, LANES)
    other = lax.ppermute(got, DP, partners(0, 1))
    parts = totals(got, other, ids)
    new_error = remainder(picks, grads, error, begun)
    parts = [parts[0]] + [swapped(parts[b], b) for b in (1, 2, 3)]
    new_params, new_momentum = update(momentum, params, parts)
    return new_error[None], new_params, new_momentum


def solution(mesh):
    return jax.shard_map(
        on_device,
        mesh=mesh,
        in_specs=(
            P(DP, None, None),
            P(DP, None, None),
            P(DP, None),
            P(DP),
            P(DP, None),
            P(DP, None),
        ),
        out_specs=(P(DP, None, None), P(DP, None), P(DP, None)),
        check_vma=False,
    )
```

```python
import jax
import jax.numpy as jnp
from jax import lax
from jax.experimental import pallas as pl
from jax.experimental.pallas import tpu as pltpu
from jax.sharding import PartitionSpec as P

DP = "dp"
PEERS = 16
LANES = 128
STEP = 1024
CHUNKS = 8
EARLY = 5
MEET = ((2, 2), (2, 2), (2, 2), (3, 3))


def rank(x, z, y, c):
    return ((x * 4 + z) * 4 + y) * 2 + c


def partners(zbits, cbits):
    ranks = range(128)
    return [(i, i ^ (zbits * 8) ^ cbits) for i in ranks]


def planes():
    cells = [(x, y) for x in range(4) for y in range(4)]
    groups = []
    for z in range(4):
        order = sorted(cells, key=lambda p: (p != MEET[z], -p[0], -p[1]))
        groups += [[rank(x, z, y, c) for x, y in order] for c in range(2)]
    return groups


def early_chunks():
    here = lax.axis_index(DP)
    far = here // 32 + here // 8 % 4 + here // 2 % 4
    return jnp.clip(EARLY - far, 0, CHUNKS)


def chunk_loads(i, grads, error, gbuf, ebuf, gsem, esem):
    rows = pl.ds(i * STEP, STEP)
    return (
        pltpu.make_async_copy(grads.at[rows], gbuf.at[rows], gsem.at[i]),
        pltpu.make_async_copy(error.at[rows], ebuf.at[rows], esem.at[i]),
    )


def chunk_store(i, obuf, out, osem):
    rows = pl.ds(i * STEP, STEP)
    return pltpu.make_async_copy(obuf.at[i, pl.ds(0, STEP)], out.at[rows], osem.at[i])


def chunk_work(i, picks, gbuf, ebuf, obuf):
    rows = pl.ds(i * STEP, STEP)
    obuf[i, pl.ds(0, STEP), :] = gbuf[rows, :] + ebuf[rows, :]
    for k in range(picks.shape[0]):
        row = picks[k] - i * STEP
        row = jnp.where((row >= 0) & (row < STEP), row, STEP)
        obuf[i, pl.ds(row, 1), :] = jnp.zeros((1, LANES), jnp.float32)


def dense_chunks(wanted, picks, grads, error, out, gbuf, ebuf, obuf, gsem, esem, osem, first):
    for i in range(CHUNKS):

        @pl.when(wanted(i))
        def _():
            for copy in chunk_loads(i, grads, error, gbuf, ebuf, gsem, esem):
                copy.start()

    first()
    for i in range(CHUNKS):

        @pl.when(wanted(i))
        def _():
            for copy in chunk_loads(i, grads, error, gbuf, ebuf, gsem, esem):
                copy.wait()
            chunk_work(i, picks, gbuf, ebuf, obuf)
            chunk_store(i, obuf, out, osem).start()

    for i in range(CHUNKS):

        @pl.when(wanted(i))
        def _():
            chunk_store(i, obuf, out, osem).wait()


def dense_scratch(blocks):
    return [
        pltpu.VMEM((blocks, LANES), jnp.float32),
        pltpu.VMEM((blocks, LANES), jnp.float32),
        pltpu.VMEM((CHUNKS, STEP + 8, LANES), jnp.float32),
        pltpu.SemaphoreType.DMA((CHUNKS,)),
        pltpu.SemaphoreType.DMA((CHUNKS,)),
        pltpu.SemaphoreType.DMA((CHUNKS,)),
    ]


def rows_kernel(
    picks_hbm, grads, error, grads_rows, error_rows, send, out,
    picks, grow, erow, psem, rsem, ssem, gbuf, ebuf, obuf, gsem, esem, osem,
):
    fetch = pltpu.make_async_copy(picks_hbm, picks, psem)
    fetch.start()
    fetch.wait()
    count = picks.shape[0]
    for k in range(count):
        row = picks[k]
        pltpu.make_async_copy(grads_rows.at[pl.ds(row, 1)], grow.at[pl.ds(k, 1)], rsem).start()
        pltpu.make_async_copy(error_rows.at[pl.ds(row, 1)], erow.at[pl.ds(k, 1)], ssem).start()
    limit = early_chunks()

    def build():
        lane = lax.broadcasted_iota(jnp.int32, (1, LANES), 1) % count
        ids = jnp.zeros((1, LANES), jnp.int32)
        for k in range(count):
            ids = jnp.where(lane == k, picks[k], ids)
        pltpu.make_async_copy(grads_rows.at[pl.ds(0, count)], grow, rsem).wait()
        pltpu.make_async_copy(error_rows.at[pl.ds(0, count)], erow, ssem).wait()
        acc = grow[:, 0, :] + erow[:, 0, :]
        ids = ids.astype(jnp.float32)
        for p in range(PEERS):
            base = p * (count + 1)
            send[base : base + count, :] = acc
            send[base + count : base + count + 1, :] = ids

    dense_chunks(
        lambda i: i < limit, picks, grads, error, out, gbuf, ebuf, obuf, gsem, esem, osem, build
    )


def chosen_rows(picks, grads, error):
    count = picks.shape[0]
    return pl.pallas_call(
        rows_kernel,
        in_specs=[pl.BlockSpec(memory_space=pltpu.HBM)] * 5,
        out_specs=[pl.BlockSpec(memory_space=pltpu.VMEM), pl.BlockSpec(memory_space=pltpu.HBM)],
        scratch_shapes=[
            pltpu.SMEM((count,), jnp.int32),
            pltpu.VMEM((count, 1, LANES), jnp.float32),
            pltpu.VMEM((count, 1, LANES), jnp.float32),
            pltpu.SemaphoreType.DMA,
            pltpu.SemaphoreType.DMA,
            pltpu.SemaphoreType.DMA,
        ]
        + dense_scratch(grads.shape[0]),
        out_shape=[
            jax.ShapeDtypeStruct((PEERS * (count + 1), LANES), jnp.float32),
            jax.ShapeDtypeStruct(grads.shape, jnp.float32),
        ],
        name="chosen_rows",
    )(picks, grads, error, grads.reshape(-1, 1, LANES), error.reshape(-1, 1, LANES))


def late_kernel(
    picks_hbm, grads, error, begun, out,
    picks, psem, gbuf, ebuf, obuf, gsem, esem, osem,
):
    limit = early_chunks()

    @pl.when(limit < CHUNKS)
    def _():
        fetch = pltpu.make_async_copy(picks_hbm, picks, psem)
        fetch.start()
        dense_chunks(
            lambda i: i >= limit,
            picks, grads, error, out, gbuf, ebuf, obuf, gsem, esem, osem, fetch.wait,
        )


def remainder(picks, grads, error, begun):
    return pl.pallas_call(
        late_kernel,
        in_specs=[pl.BlockSpec(memory_space=pltpu.HBM)] * 4,
        out_specs=pl.BlockSpec(memory_space=pltpu.HBM),
        out_shape=jax.ShapeDtypeStruct(grads.shape, jnp.float32),
        input_output_aliases={3: 0},
        scratch_shapes=[pltpu.SMEM(picks.shape, jnp.int32), pltpu.SemaphoreType.DMA]
        + dense_scratch(grads.shape[0]),
        cost_estimate=pl.CostEstimate(
            flops=40_000_000, bytes_accessed=12 << 20, transcendentals=0
        ),
        name="remainder",
    )(picks, grads, error, begun)


def totals_kernel(mine, other, id0, id1, id2, id3, out0, out1, out2, out3):
    count = mine.shape[0] // PEERS - 1
    per = LANES // count
    lane = lax.broadcasted_iota(jnp.int32, (1, LANES), 1)
    slots = id0.shape[1]
    columns = []
    for ids in (id0, id1, id2, id3):
        wide = jnp.broadcast_to(ids[...].astype(jnp.float32), (LANES, slots))
        columns.append(wide.T)
    owned = jnp.concatenate(columns, axis=0)
    marks, values = [], []
    for g in range(2 * PEERS // per):
        ids = None
        got = mine if g < PEERS // per else other
        for q in range(per):
            base = (g * per + q) % PEERS * (count + 1)
            row = got[base + count : base + count + 1, :]
            ids = row if ids is None else jnp.where(lane < q * count, ids, row)
            values.append(got[base : base + count, :])
        marks.append(jnp.where(owned == ids, 1.0, 0.0).astype(jnp.bfloat16))
    marks = jnp.concatenate(marks, axis=1)
    values = jnp.concatenate(values, axis=0)
    total = None
    for _ in range(3):
        part = values.astype(jnp.bfloat16)
        values = values - part.astype(jnp.float32)
        term = jnp.dot(marks, part, preferred_element_type=jnp.float32)
        total = term if total is None else total + term
    for j, out in enumerate((out0, out1, out2, out3)):
        out[...] = total[j * slots : (j + 1) * slots, :]


def totals(mine, other, ids):
    slots = ids[0].shape[1]
    return pl.pallas_call(
        totals_kernel,
        out_shape=[jax.ShapeDtypeStruct((slots, LANES), jnp.float32)] * 4,
        compiler_params=pltpu.CompilerParams(vmem_limit_bytes=8 << 20),
        name="totals",
    )(mine, other, *ids)


def update_kernel(momentum, params, a, b, c, d, new_params, new_momentum):
    fresh = 0.9 * momentum[...] + ((a[...] + b[...]) + (c[...] + d[...]))
    new_momentum[...] = fresh
    new_params[...] = params[...] - 0.5 * fresh


def update(momentum, params, parts):
    shape = jax.ShapeDtypeStruct(params.shape, jnp.float32)
    return pl.pallas_call(
        update_kernel,
        out_shape=[shape, shape],
        compiler_params=pltpu.CompilerParams(vmem_limit_bytes=2 << 20),
        name="update",
    )(momentum, params, *parts)


def swapped(x, bits):
    return lax.ppermute(x, DP, partners(bits, 0))


def on_device(grads, error, picks, owned_ids, params, momentum):
    return step(grads[0], error[0], picks[0], owned_ids, params, momentum)


def step(grads, error, picks, owned_ids, params, momentum):
    count = picks.shape[0]
    send, begun = chosen_rows(picks, grads, error)
    send = send.reshape(PEERS, count + 1, 1, LANES)
    got = lax.all_to_all(send, DP, 0, 0, tiled=True, axis_index_groups=planes())
    mine = owned_ids.reshape(1, -1)
    ids = [mine] + [swapped(mine, b) for b in (1, 2, 3)]
    got = got.reshape(-1, LANES)
    other = lax.ppermute(got, DP, partners(0, 1))
    parts = totals(got, other, ids)
    new_error = remainder(picks, grads, error, begun)
    parts = [parts[0]] + [swapped(parts[b], b) for b in (1, 2, 3)]
    new_params, new_momentum = update(momentum, params, parts)
    return new_error[None], new_params, new_momentum


def solution(mesh):
    return jax.shard_map(
        on_device,
        mesh=mesh,
        in_specs=(
            P(DP, None, None),
            P(DP, None, None),
            P(DP, None),
            P(DP),
            P(DP, None),
            P(DP, None),
        ),
        out_specs=(P(DP, None, None), P(DP, None), P(DP, None)),
        check_vma=False,
    )
```
